32 devices in a mesh: gx: 8 (over y, x, core), gy: 4 (over z).
Axes of the slice: x: 2, y: 2, z: 4, core: 2. Of those that a mesh axis runs over, the one named last changes fastest.
Arguments:
- products: bfloat16 [1536, 3, 2048], P('gy', None, 'gx'), may hold values from -6 to 6
- operator: bfloat16 [1536, 1536], P(None, 'gy'), may hold values from -0.21875 to 0.21875
Outputs:
- derivative: bfloat16 [1536, 3, 2048], P(('gy', 'gx'))
The draws below stay inside these ranges and needn't reach their ends.
All inputs are finite; a program needn't handle non-finite values.
Results may differ from the reference program's by a relative error of at most 0.002.
Values may be sent and summed in bfloat16 or wider, within the bound.
A program may use at most 64 MiB of HBM per device.

```python
import jax
import jax.numpy as jnp

NY = 1536
MODES = 2048


def strengthened(array, own_key, source, target, blocks, factor):
    owner, partner = [(jnp.arange(array.shape[position]) // (array.shape[position] // blocks)).reshape([-1 if axis == position else 1 for axis in range(array.ndim)]) for position in (source, target)]
    chosen = jax.random.permutation(own_key, blocks)[partner]
    strong = (owner == chosen) | (owner == (partner + blocks // 2) % blocks)
    return jnp.where(strong, factor * array, array)


def block_scale(rng, shape, pieces, smallest, largest):
    loudness = 1.0
    for axis_at, shards_of in pieces:
        heights = jax.random.uniform(jax.random.fold_in(jax.random.fold_in(rng, 6), axis_at), (shards_of,), jnp.float32, smallest / len(pieces), largest / len(pieces))
        loudness = loudness * jnp.repeat(jnp.exp(heights), shape[axis_at] // shards_of).reshape((-1,) + (1,) * (len(shape) - 1 - axis_at))
    return loudness


def gaussian(own_key, extent, scale, limit, split=(), kind=jnp.bfloat16):
    entries = scale * jax.random.normal(own_key, extent, jnp.float32)
    if split:
        entries = entries * block_scale(own_key, extent, split, -0.22, 0.18)
    return jnp.clip(entries, -limit, limit).astype(kind)


def heavy_noise(key, shape, width, limit, pieces, heavy, kind=jnp.bfloat16):
    entries = width * jax.random.normal(key, shape, jnp.float32)
    if pieces:
        entries = entries * block_scale(key, shape, pieces, -0.22, 0.18)
    return jnp.clip(strengthened(entries, jax.random.fold_in(key, 3), *heavy), -limit, limit).astype(kind)


def setup_inputs(seed: int = 0) -> dict:
    streams_of = jax.random.split(jax.random.key(seed), 3)
    products = gaussian(streams_of[0], (NY, 3, MODES), 1.0, 6.0, ((0, 4), (2, 8)))
    operator = heavy_noise(streams_of[1], (NY, NY), NY ** -0.5, 0.21875, ((1, 4),), (1, 0, 4, 2.0))
    return dict(products=products, operator=operator)


def reference(products, operator):
    flat = products.reshape(NY, 3 * MODES)
    summed = jnp.dot(operator, flat, preferred_element_type=jnp.float32)
    return summed.astype(jnp.bfloat16).reshape(NY, 3, MODES)
```

```python
import functools

import jax
import jax.numpy as jnp
from jax import lax
from jax.experimental import pallas as pl
from jax.experimental.pallas import tpu as pltpu
from jax.sharding import PartitionSpec as P

MESH = pl.DeviceIdType.MESH
LANES = 128
SUBLANES = 16
VMEM_BYTES = 60 * 1024 * 1024


def kernel(n, g, parts, p_ref, op_ref, out_ref, blocks, ops, res,
           own_send, fwd_send, op_send, spread_send, res_send, blk_recv, op_recv, out_recv):
    j, k = lax.axis_index("gx"), lax.axis_index("gy")
    half = n // 2
    side = lax.div(k, half)
    step = 1 - 2 * side
    centre = jnp.where(side == 0, half - 1, half)
    other = n - 1 - centre
    is_centre = k == centre
    planes, rows, cols = p_ref.shape
    width = cols // parts
    chunks = planes * parts
    piece = half * rows // g
    outrows = rows // g

    def near(d):
        return centre - step * d

    def far(d):
        return other + step * d

    barrier = pltpu.get_barrier_semaphore()
    greeted = 0
    for dk in range(half):
        kk = side * half + lax.rem(k - side * half + dk, half)
        for dj in range(g):
            if dk or dj:
                pl.semaphore_signal(barrier, inc=1, device_id=(lax.rem(j + dj, g), kk), device_id_type=MESH)
                greeted += 1
    for dk in range(half):
        pl.semaphore_signal(barrier, inc=1, device_id=(j, (1 - side) * half + dk), device_id_type=MESH)
        greeted += 1
    pl.semaphore_wait(barrier, greeted)

    def remote(src, dst, send, recv, gx, gy):
        return pltpu.make_async_remote_copy(
            src_ref=src, dst_ref=dst, send_sem=send, recv_sem=recv,
            device_id=(gx, gy), device_id_type=MESH)

    def wait_bytes(ref, sem):
        pltpu.make_async_copy(ref, ref, sem).wait()

    def chunk_of(ref, i):
        c, h = lax.div(i, parts), lax.rem(i, parts)
        return ref.at[c, :, pl.ds(pl.multiple_of(h * width, width), width)]

    def piece_rows(at):
        return pl.ds(pl.multiple_of(at * piece, piece), piece)

    def op_out(slot, to_side, to):
        at = pl.multiple_of(to_side * (half * rows) + j * piece, piece)
        remote(op_ref.at[pl.ds(at, piece), :], ops.at[k, piece_rows(j), :],
               op_send.at[slot], op_recv.at[k, j], j, to).start()

    def block_out(to):
        for i in range(chunks):
            remote(chunk_of(p_ref, i), chunk_of(blocks.at[k], i), own_send, blk_recv.at[k, i], j, to).start()

    @pl.when(is_centre)
    def _():
        op_out(0, 1 - side, other)
        block_out(other)

        sources = [near(d) for d in range(1, half)] + [far(d) for d in range(half)]
        sibling = j + 1 - 2 * lax.rem(j, 2)

        def spread(s, at, to):
            part = ops.at[s, piece_rows(at), :]
            remote(part, part, spread_send.at[s], op_recv.at[s, at], to, k).start()

        def arrived(s, at):
            part = ops.at[s, piece_rows(at), :]
            wait_bytes(part, op_recv.at[s, at])

        for s in sources:
            arrived(s, j)
            for d in range(1, g // 2):
                spread(s, j, lax.rem(j + 2 * d, g))
            spread(s, j, sibling)
        for s in sources:
            for d in range(1, g // 2):
                at = lax.rem(j + 2 * d, g)
                arrived(s, at)
                spread(s, at, sibling)
        for i in range(chunks):
            for d in range(1, half):
                s = near(d)
                part = chunk_of(blocks.at[s], i)
                wait_bytes(part, blk_recv.at[s, i])
                remote(part, part, fwd_send.at[d - 1], blk_recv.at[s, i], j, other).start()
        for s in sources:
            for d in range(g // 2):
                arrived(s, lax.rem(sibling + 2 * d, g))

        def one(i, carry):
            c, h = lax.div(i, parts), lax.rem(i, parts)
            lane = pl.ds(pl.multiple_of(h * width, width), width)
            for d in range(half):
                part = chunk_of(blocks.at[far(d)], i)
                wait_bytes(part, blk_recv.at[far(d), i])
            target = pl.ds(pl.multiple_of(j * cols + h * width, width), width)
            for d in reversed(range(half)):
                at = pl.multiple_of(near(d) * rows, rows)
                rel = pl.multiple_of((near(d) - side * half) * rows, rows)
                total = jnp.dot(op_ref[pl.ds(at, rows), :], p_ref[c, :, lane], preferred_element_type=jnp.float32)
                for s in sources:
                    total += jnp.dot(ops[s, pl.ds(rel, rows), :], blocks[s, c, :, lane],
                                     preferred_element_type=jnp.float32)
                res[d, c, :, lane] = total.astype(res.dtype)
                for dj in range(1, g) if d == 0 else range(g):
                    to = lax.rem(j + dj, g)
                    remote(res.at[d, c, pl.ds(pl.multiple_of(to * outrows, outrows), outrows), lane],
                           out_ref.at[c, :, target], res_send.at[d], out_recv, to, near(d)).start()
                if d == 0:
                    pltpu.make_async_copy(
                        res.at[d, c, pl.ds(pl.multiple_of(j * outrows, outrows), outrows), lane],
                        out_ref.at[c, :, target], out_recv).start()
            return carry

        lax.fori_loop(0, chunks, one, 0)
        wait_bytes(ops.at[0, piece_rows(0), :], op_send.at[0])
        wait_bytes(p_ref, own_send)
        for d in range(1, half):
            wait_bytes(blocks.at[near(d)], fwd_send.at[d - 1])
        for s in sources:
            for _ in range(1):
                wait_bytes(ops.at[s, pl.ds(0, (g - 1) * piece), :], spread_send.at[s])
        for d in range(half):
            sent = rows - outrows if d == 0 else rows
            wait_bytes(res.at[d, :, pl.ds(0, sent), :], res_send.at[d])

    @pl.when(jnp.logical_not(is_centre))
    def _():
        op_out(0, 1 - side, other)
        op_out(1, side, centre)
        block_out(centre)
        wait_bytes(ops.at[0, piece_rows(0), :], op_send.at[0])
        wait_bytes(ops.at[0, piece_rows(0), :], op_send.at[1])
        wait_bytes(p_ref, own_send)

    wait_bytes(out_ref, out_recv)


def at_centres(n, g, products, operator):
    rows, planes, cols = products.shape
    parts = 2 if cols % (2 * LANES) == 0 else 1
    half = n // 2
    chunks = planes * parts
    out = pl.pallas_call(
        functools.partial(kernel, n, g, parts),
        out_shape=jax.ShapeDtypeStruct((planes, rows // g, cols * g), jnp.bfloat16),
        in_specs=[pl.BlockSpec(memory_space=pltpu.VMEM)] * 2,
        out_specs=pl.BlockSpec(memory_space=pltpu.VMEM),
        scratch_shapes=[
            pltpu.VMEM((n, planes, rows, cols), jnp.bfloat16),
            pltpu.VMEM((n, half * rows, rows), jnp.bfloat16),
            pltpu.VMEM((half, planes, rows, cols), jnp.bfloat16),
            pltpu.SemaphoreType.DMA,
            pltpu.SemaphoreType.DMA((half,)),
            pltpu.SemaphoreType.DMA((2,)),
            pltpu.SemaphoreType.DMA((n,)),
            pltpu.SemaphoreType.DMA((half,)),
            pltpu.SemaphoreType.DMA((n, chunks)),
            pltpu.SemaphoreType.DMA((n, g)),
            pltpu.SemaphoreType.DMA,
        ],
        compiler_params=pltpu.CompilerParams(
            collective_id=0, has_side_effects=True, vmem_limit_bytes=VMEM_BYTES),
    )(products.transpose(1, 0, 2), operator)
    return out.transpose(1, 0, 2)


def by_collectives(products, operator):
    y_local, three, m_local = products.shape
    flat = products.reshape(y_local, three * m_local)
    summed = lax.psum_scatter(
        jnp.dot(operator, flat, preferred_element_type=jnp.float32), "gy", scatter_dimension=0, tiled=True)
    result = summed.astype(jnp.bfloat16).reshape(y_local, three, m_local)
    return lax.all_to_all(result, "gx", split_axis=0, concat_axis=2, tiled=True)


def solution(mesh):
    n, g = mesh.shape["gy"], mesh.shape["gx"]

    def body(products, operator):
        rows, planes, cols = products.shape
        aligned = (n % 2 == 0 and g % 2 == 0 and rows % (g * SUBLANES) == 0
                   and rows % LANES == 0 and cols % LANES == 0)
        held = 2 * (products.size * (n + n // 2 + 2) + operator.size * (1 + n // 2))
        if aligned and held < VMEM_BYTES // 2:
            return at_centres(n, g, products, operator)
        return by_collectives(products, operator)

    return jax.shard_map(
        body,
        mesh=mesh,
        in_specs=(P("gy", None, "gx"), P(None, "gy")),
        out_specs=P(("gy", "gx"), None, None),
        check_vma=False,
    )
```

```python
import functools

import jax
import jax.numpy as jnp
from jax import lax
from jax.experimental import pallas as pl
from jax.experimental.pallas import tpu as pltpu
from jax.sharding import PartitionSpec as P

MESH = pl.DeviceIdType.MESH
LANES = 128
SUBLANES = 16
VMEM_BYTES = 60 * 1024 * 1024
GRANT = 54500 * 1024


def kernel(n, g, parts, p_ref, op_ref, out_ref, blocks, ops, res,
           own_send, fwd_send, op_send, spread_send, res_send, blk_recv, op_recv, out_recv, own_copy, ready):
    j, k = lax.axis_index("gx"), lax.axis_index("gy")
    half = n // 2
    side = lax.div(k, half)
    step = 1 - 2 * side
    centre = jnp.where(side == 0, half - 1, half)
    other = n - 1 - centre
    is_centre = k == centre
    planes, rows, cols = p_ref.shape
    width = cols // parts
    chunks = planes * parts
    piece = half * rows // g
    outrows = rows // g
    ahead, lead = 2, 2 * chunks // 3

    def flip(mask):
        to = j
        for bit in (1 << b for b in range(mask.bit_length())):
            if mask & bit:
                to = to + bit * (1 - 2 * lax.rem(lax.div(j, bit), 2))
        return to

    def near(d):
        return centre - step * d

    def far(d):
        return other + step * d

    rounds = g.bit_length() - 1
    barrier = pltpu.get_barrier_semaphore()

    def signal(sem, gx, gy):
        pl.semaphore_signal(sem, inc=1, device_id=(gx, gy), device_id_type=MESH)

    for b in range(rounds):
        signal(barrier, flip(1 << b), k)

    @pl.when(is_centre)
    def _():
        signal(barrier, j, other)
        for d in range(1, half):
            signal(barrier, j, near(d))
        pl.semaphore_wait(barrier, rounds + half)

    @pl.when(jnp.logical_not(is_centre))
    def _():
        signal(barrier, j, centre)
        pl.semaphore_wait(barrier, rounds + 1)

    def plane_entered():
        for b in range(rounds):
            signal(ready.at[b], flip(1 << b), k)
            pl.semaphore_wait(ready.at[b], 1)

    def remote(src, dst, send, recv, gx, gy):
        return pltpu.make_async_remote_copy(
            src_ref=src, dst_ref=dst, send_sem=send, recv_sem=recv,
            device_id=(gx, gy), device_id_type=MESH)

    def wait_bytes(ref, sem):
        pltpu.make_async_copy(ref, ref, sem).wait()

    def chunk_of(ref, i):
        c, h = lax.div(i, parts), lax.rem(i, parts)
        return ref.at[c, :, pl.ds(pl.multiple_of(h * width, width), width)]

    def piece_rows(at):
        return pl.ds(pl.multiple_of(at * piece, piece), piece)

    def from_source(s):
        return pl.ds(pl.multiple_of(s * rows, rows), rows)

    def op_part(s, at):
        return ops.at[piece_rows(at), from_source(s)]

    def block_part(s, i):
        c, h = lax.div(i, parts), lax.rem(i, parts)
        return blocks.at[c, from_source(s), pl.ds(pl.multiple_of(h * width, width), width)]

    def op_out(slot, to_side, to):
        at = pl.multiple_of(to_side * (half * rows) + j * piece, piece)
        remote(op_ref.at[pl.ds(at, piece), :], op_part(k, j),
               op_send.at[slot], op_recv.at[k, j], j, to).start()

    def block_out(i, to):
        remote(chunk_of(p_ref, i), block_part(k, i), own_send, blk_recv.at[k, i], j, to).start()

    @pl.when(is_centre)
    def _():
        op_out(0, 1 - side, other)
        for i in range(ahead):
            block_out(i, other)
        for d in range(1, half):
            signal(ready.at[rounds], j, near(d))
        own_rows = pl.ds(pl.multiple_of(side * (half * rows), half * rows), half * rows)
        own_ops = pltpu.make_async_copy(op_ref.at[own_rows, :], ops.at[:, from_source(k)], own_copy.at[0])
        own_ops.start()
        own_blocks = pltpu.make_async_copy(p_ref, blocks.at[:, from_source(k), :], own_copy.at[1])
        own_blocks.start()

        plane_entered()
        pl.semaphore_wait(ready.at[rounds], half - 1)

        sources = [near(d) for d in range(1, half)] + [far(d) for d in range(half)]
        sibling = flip(1)

        def spread(s, at, to):
            part = op_part(s, at)
            remote(part, part, spread_send.at[s], op_recv.at[s, at], to, k).start()

        def arrived(s, at):
            part = op_part(s, at)
            wait_bytes(part, op_recv.at[s, at])

        for s in sources:
            arrived(s, j)
            for d in range(1, g // 2):
                spread(s, j, flip(2 * d))
            spread(s, j, sibling)
        def forward(i):
            for d in range(1, half):
                part = block_part(near(d), i)
                wait_bytes(part, blk_recv.at[near(d), i])
                remote(part, part, fwd_send.at[d - 1], blk_recv.at[near(d), i], j, other).start()

        for i in range(lead):
            forward(i)
            if i + ahead < chunks:
                block_out(i + ahead, other)
        for i in range(lead + ahead, chunks):
            block_out(i, other)
        for s in sources:
            for d in range(1, g // 2):
                at = flip(2 * d)
                arrived(s, at)
                spread(s, at, sibling)
        for s in sources:
            for d in range(g // 2):
                arrived(s, flip(2 * d + 1))
        own_ops.wait()
        own_blocks.wait()

        def one(i, carry):
            c, h = lax.div(i, parts), lax.rem(i, parts)
            lane = pl.ds(pl.multiple_of(h * width, width), width)

            @pl.when(i + lead < chunks)
            def _():
                forward(i + lead)

            for d in range(half):
                wait_bytes(block_part(far(d), i), blk_recv.at[far(d), i])
            target = pl.ds(pl.multiple_of(j * cols + h * width, width), width)
            for d in reversed(range(half)):
                rel = pl.multiple_of((near(d) - side * half) * rows, rows)
                total = jnp.dot(ops[pl.ds(rel, rows), :], blocks[c, :, lane], preferred_element_type=jnp.float32)
                res[d, c, :, lane] = total.astype(res.dtype)
                for mask in reversed(range(1 if d == 0 else 0, g)):
                    to = flip(mask)
                    remote(res.at[d, c, pl.ds(pl.multiple_of(to * outrows, outrows), outrows), lane],
                           out_ref.at[c, :, target], res_send.at[d], out_recv, to, near(d)).start()
                if d == 0:
                    pltpu.make_async_copy(
                        res.at[d, c, pl.ds(pl.multiple_of(j * outrows, outrows), outrows), lane],
                        out_ref.at[c, :, target], out_recv).start()
            return carry

        lax.fori_loop(0, chunks, one, 0)
        wait_bytes(op_part(0, 0), op_send.at[0])
        wait_bytes(blocks.at[:, from_source(0), :], own_send)
        for d in range(1, half):
            wait_bytes(blocks.at[:, from_source(0), :], fwd_send.at[d - 1])
        for s in sources:
            wait_bytes(ops.at[pl.ds(0, (g - 1) * piece), from_source(0)], spread_send.at[s])
        for d in range(half):
            sent = rows - outrows if d == 0 else rows
            wait_bytes(res.at[d, :, pl.ds(0, sent), :], res_send.at[d])

    @pl.when(jnp.logical_not(is_centre))
    def _():
        op_out(1, side, centre)
        block_out(0, centre)
        pl.semaphore_wait(ready.at[rounds], 1)
        op_out(0, 1 - side, other)
        for i in range(1, chunks):
            block_out(i, centre)
        plane_entered()
        signal(ready.at[rounds], j, centre)
        wait_bytes(op_part(0, 0), op_send.at[0])
        wait_bytes(op_part(0, 0), op_send.at[1])
        wait_bytes(blocks.at[:, from_source(0), :], own_send)

    wait_bytes(out_ref, out_recv)


def at_centres(n, g, products, operator):
    rows, planes, cols = products.shape
    parts = 2 if cols % (2 * LANES) == 0 else 1
    half = n // 2
    chunks = planes * parts
    out = pl.pallas_call(
        functools.partial(kernel, n, g, parts),
        out_shape=jax.ShapeDtypeStruct((planes, rows // g, cols * g), jnp.bfloat16),
        in_specs=[pl.BlockSpec(memory_space=pl.ANY)] * 2,
        out_specs=pl.BlockSpec(memory_space=pl.ANY),
        scratch_shapes=[
            pltpu.VMEM((planes, n * rows, cols), jnp.bfloat16),
            pltpu.VMEM((half * rows, n * rows), jnp.bfloat16),
            pltpu.VMEM((half, planes, rows, cols), jnp.bfloat16),
            pltpu.SemaphoreType.DMA,
            pltpu.SemaphoreType.DMA((half,)),
            pltpu.SemaphoreType.DMA((2,)),
            pltpu.SemaphoreType.DMA((n,)),
            pltpu.SemaphoreType.DMA((half,)),
            pltpu.SemaphoreType.DMA((n, chunks)),
            pltpu.SemaphoreType.DMA((n, g)),
            pltpu.SemaphoreType.DMA,
            pltpu.SemaphoreType.DMA((2,)),
            pltpu.SemaphoreType.REGULAR((g.bit_length(),)),
        ],
        compiler_params=pltpu.CompilerParams(
            collective_id=0, has_side_effects=True, vmem_limit_bytes=GRANT),
    )(products.transpose(1, 0, 2), operator)
    return out.transpose(1, 0, 2)


def by_collectives(products, operator):
    y_local, three, m_local = products.shape
    flat = products.reshape(y_local, three * m_local)
    summed = lax.psum_scatter(
        jnp.dot(operator, flat, preferred_element_type=jnp.float32), "gy", scatter_dimension=0, tiled=True)
    result = summed.astype(jnp.bfloat16).reshape(y_local, three, m_local)
    return lax.all_to_all(result, "gx", split_axis=0, concat_axis=2, tiled=True)


def solution(mesh):
    n, g = mesh.shape["gy"], mesh.shape["gx"]

    def body(products, operator):
        rows, planes, cols = products.shape
        aligned = (n % 2 == 0 and g & (g - 1) == 0 and g > 1 and rows % (g * SUBLANES) == 0
                   and rows % LANES == 0 and cols % LANES == 0)
        held = 2 * (products.size * (n + n // 2 + 2) + operator.size * (1 + n // 2))
        if aligned and held < VMEM_BYTES // 2:
            return at_centres(n, g, products, operator)
        return by_collectives(products, operator)

    return jax.shard_map(
        body,
        mesh=mesh,
        in_specs=(P("gy", None, "gx"), P(None, "gy")),
        out_specs=P(("gy", "gx"), None, None),
        check_vma=False,
    )
```

```python
import functools

import jax
import jax.numpy as jnp
from jax import lax
from jax.experimental import pallas as pl
from jax.experimental.pallas import tpu as pltpu
from jax.sharding import PartitionSpec as P

MESH = pl.DeviceIdType.MESH
LANES = 128
SUBLANES = 16
VMEM_BYTES = 60 * 1024 * 1024
GRANT = 54500 * 1024


def kernel(n, g, parts, p_ref, op_ref, out_ref, blocks, ops, res,
           own_send, fwd_send, op_send, spread_send, res_send, blk_recv, op_recv, out_recv, own_copy, ready, ahead_of):
    j, k = lax.axis_index("gx"), lax.axis_index("gy")
    half = n // 2
    side = lax.div(k, half)
    step = 1 - 2 * side
    centre = jnp.where(side == 0, half - 1, half)
    other = n - 1 - centre
    is_centre = k == centre
    planes, rows, cols = p_ref.shape
    width = cols // parts
    chunks = planes * parts
    piece = half * rows // g
    outrows = rows // g
    ahead, lead = 2, chunks - 1

    def flip(mask):
        to = j
        for bit in (1 << b for b in range(mask.bit_length())):
            if mask & bit:
                to = to + bit * (1 - 2 * lax.rem(lax.div(j, bit), 2))
        return to

    def near(d):
        return centre - step * d

    def far(d):
        return other + step * d

    rounds = g.bit_length() - 1
    barrier = pltpu.get_barrier_semaphore()

    def signal(sem, gx, gy):
        pl.semaphore_signal(sem, inc=1, device_id=(gx, gy), device_id_type=MESH)

    for b in range(rounds):
        signal(barrier, flip(1 << b), k)

    @pl.when(is_centre)
    def _():
        signal(barrier, j, other)
        for d in range(1, half):
            signal(barrier, j, near(d))
        pl.semaphore_wait(barrier, rounds + half)

    @pl.when(jnp.logical_not(is_centre))
    def _():
        signal(barrier, j, centre)
        pl.semaphore_wait(barrier, rounds + 1)

    def plane_entered():
        for b in range(rounds):
            signal(ready.at[b], flip(1 << b), k)
            pl.semaphore_wait(ready.at[b], 1)

    def remote(src, dst, send, recv, gx, gy):
        return pltpu.make_async_remote_copy(
            src_ref=src, dst_ref=dst, send_sem=send, recv_sem=recv,
            device_id=(gx, gy), device_id_type=MESH)

    def wait_bytes(ref, sem):
        pltpu.make_async_copy(ref, ref, sem).wait()

    def chunk_of(ref, i):
        c, h = lax.div(i, parts), lax.rem(i, parts)
        return ref.at[c, :, pl.ds(pl.multiple_of(h * width, width), width)]

    def piece_rows(at):
        return pl.ds(pl.multiple_of(at * piece, piece), piece)

    def from_source(s):
        return pl.ds(pl.multiple_of(s * rows, rows), rows)

    def op_part(s, at):
        return ops.at[piece_rows(at), from_source(s)]

    def block_part(s, i):
        c, h = lax.div(i, parts), lax.rem(i, parts)
        return blocks.at[c, from_source(s), pl.ds(pl.multiple_of(h * width, width), width)]

    def op_out(slot, to_side, to):
        at = pl.multiple_of(to_side * (half * rows) + j * piece, piece)
        remote(op_ref.at[pl.ds(at, piece), :], op_part(k, j),
               op_send.at[slot], op_recv.at[k, j], j, to).start()

    def block_out(i, to):
        remote(chunk_of(p_ref, i), block_part(k, i), own_send, blk_recv.at[k, i], j, to).start()

    @pl.when(is_centre)
    def _():
        op_out(0, 1 - side, other)
        for i in range(ahead):
            block_out(i, other)
        for d in range(1, half):
            signal(ready.at[rounds], j, near(d))
        own_rows = pl.ds(pl.multiple_of(side * (half * rows), half * rows), half * rows)
        own_ops = pltpu.make_async_copy(op_ref.at[own_rows, :], ops.at[:, from_source(k)], own_copy.at[0])
        own_ops.start()
        own_blocks = pltpu.make_async_copy(p_ref, blocks.at[:, from_source(k), :], own_copy.at[1])
        own_blocks.start()

        plane_entered()
        pl.semaphore_wait(ready.at[rounds], half - 1)

        sources = [near(d) for d in range(1, half)] + [far(d) for d in range(half)]
        sibling = flip(1)

        def spread(s, at, to):
            part = op_part(s, at)
            remote(part, part, spread_send.at[s], op_recv.at[s, at], to, k).start()

        def arrived(s, at):
            part = op_part(s, at)
            wait_bytes(part, op_recv.at[s, at])

        for s in sources:
            arrived(s, j)
            for d in range(1, g // 2):
                spread(s, j, flip(2 * d))
            spread(s, j, sibling)
        def forward(i):
            for d in range(1, half):
                part = block_part(near(d), i)
                wait_bytes(part, blk_recv.at[near(d), i])
                remote(part, part, fwd_send.at[d - 1], blk_recv.at[near(d), i], j, other).start()

        for i in range(lead):
            forward(i)
            if i + ahead < lead:
                block_out(i + ahead, other)
        block_out(lead, other)
        for s in sources:
            for d in range(1, g // 2):
                at = flip(2 * d)
                arrived(s, at)
                spread(s, at, sibling)
        for s in sources:
            for d in range(g // 2):
                arrived(s, flip(2 * d + 1))
        own_ops.wait()
        own_blocks.wait()

        def one(i, carry):
            c, h = lax.div(i, parts), lax.rem(i, parts)
            lane = pl.ds(pl.multiple_of(h * width, width), width)

            @pl.when(i + lead < chunks)
            def _():
                forward(i + lead)

            last = far(half - 1)
            others = pl.ds(pl.multiple_of(side * rows, rows), (n - 1) * rows)
            for d in range(half - 1):
                wait_bytes(block_part(far(d), i), blk_recv.at[far(d), i])
            ahead_of[...] = jnp.dot(ops[:, others], blocks[c, others, lane], preferred_element_type=jnp.float32)
            wait_bytes(block_part(last, i), blk_recv.at[last, i])
            target = pl.ds(pl.multiple_of(j * cols + h * width, width), width)
            for d in reversed(range(half)):
                rel = pl.multiple_of((near(d) - side * half) * rows, rows)
                total = ahead_of[pl.ds(rel, rows), :] + jnp.dot(
                    ops[pl.ds(rel, rows), from_source(last)], blocks[c, from_source(last), lane],
                    preferred_element_type=jnp.float32)
                res[d, c, :, lane] = total.astype(res.dtype)
                for mask in reversed(range(1 if d == 0 else 0, g)):
                    to = flip(mask)
                    remote(res.at[d, c, pl.ds(pl.multiple_of(to * outrows, outrows), outrows), lane],
                           out_ref.at[c, :, target], res_send.at[d], out_recv, to, near(d)).start()
                if d == 0:
                    pltpu.make_async_copy(
                        res.at[d, c, pl.ds(pl.multiple_of(j * outrows, outrows), outrows), lane],
                        out_ref.at[c, :, target], out_recv).start()
            return carry

        lax.fori_loop(0, chunks, one, 0)
        wait_bytes(op_part(0, 0), op_send.at[0])
        wait_bytes(blocks.at[:, from_source(0), :], own_send)
        for d in range(1, half):
            wait_bytes(blocks.at[:, from_source(0), :], fwd_send.at[d - 1])
        for s in sources:
            wait_bytes(ops.at[pl.ds(0, (g - 1) * piece), from_source(0)], spread_send.at[s])
        for d in range(half):
            sent = rows - outrows if d == 0 else rows
            wait_bytes(res.at[d, :, pl.ds(0, sent), :], res_send.at[d])

    @pl.when(jnp.logical_not(is_centre))
    def _():
        op_out(1, side, centre)
        block_out(0, centre)
        pl.semaphore_wait(ready.at[rounds], 1)
        op_out(0, 1 - side, other)
        for i in range(1, chunks):
            block_out(i, centre)
        plane_entered()
        signal(ready.at[rounds], j, centre)
        wait_bytes(op_part(0, 0), op_send.at[0])
        wait_bytes(op_part(0, 0), op_send.at[1])
        wait_bytes(blocks.at[:, from_source(0), :], own_send)

    wait_bytes(out_ref, out_recv)


def at_centres(n, g, products, operator):
    rows, planes, cols = products.shape
    parts = 2 if cols % (2 * LANES) == 0 else 1
    half = n // 2
    chunks = planes * parts
    out = pl.pallas_call(
        functools.partial(kernel, n, g, parts),
        out_shape=jax.ShapeDtypeStruct((planes, rows // g, cols * g), jnp.bfloat16),
        in_specs=[pl.BlockSpec(memory_space=pl.ANY)] * 2,
        out_specs=pl.BlockSpec(memory_space=pl.ANY),
        scratch_shapes=[
            pltpu.VMEM((planes, n * rows, cols), jnp.bfloat16),
            pltpu.VMEM((half * rows, n * rows), jnp.bfloat16),
            pltpu.VMEM((half, planes, rows, cols), jnp.bfloat16),
            pltpu.SemaphoreType.DMA,
            pltpu.SemaphoreType.DMA((half,)),
            pltpu.SemaphoreType.DMA((2,)),
            pltpu.SemaphoreType.DMA((n,)),
            pltpu.SemaphoreType.DMA((half,)),
            pltpu.SemaphoreType.DMA((n, chunks)),
            pltpu.SemaphoreType.DMA((n, g)),
            pltpu.SemaphoreType.DMA,
            pltpu.SemaphoreType.DMA((2,)),
            pltpu.SemaphoreType.REGULAR((g.bit_length(),)),
            pltpu.VMEM((half * rows, cols // parts), jnp.float32),
        ],
        compiler_params=pltpu.CompilerParams(
            collective_id=0, has_side_effects=True, vmem_limit_bytes=GRANT),
    )(products.transpose(1, 0, 2), operator)
    return out.transpose(1, 0, 2)


def by_collectives(products, operator):
    y_local, three, m_local = products.shape
    flat = products.reshape(y_local, three * m_local)
    summed = lax.psum_scatter(
        jnp.dot(operator, flat, preferred_element_type=jnp.float32), "gy", scatter_dimension=0, tiled=True)
    result = summed.astype(jnp.bfloat16).reshape(y_local, three, m_local)
    return lax.all_to_all(result, "gx", split_axis=0, concat_axis=2, tiled=True)


def solution(mesh):
    n, g = mesh.shape["gy"], mesh.shape["gx"]

    def body(products, operator):
        rows, planes, cols = products.shape
        aligned = (n % 2 == 0 and planes > 2 and g & (g - 1) == 0 and g > 1 and rows % (g * SUBLANES) == 0
                   and rows % LANES == 0 and cols % LANES == 0)
        held = 2 * (products.size * (n + n // 2 + 2) + operator.size * (1 + n // 2))
        if aligned and held < VMEM_BYTES // 2:
            return at_centres(n, g, products, operator)
        return by_collectives(products, operator)

    return jax.shard_map(
        body,
        mesh=mesh,
        in_specs=(P("gy", None, "gx"), P(None, "gy")),
        out_specs=P(("gy", "gx"), None, None),
        check_vma=False,
    )
```
